256 devices in a mesh: rep: 2 (over y), grp: 16 (over z), tp: 4 (over x), sub: 2 (over core).
Axes of the slice: x: 4, y: 2, z: 16, core: 2. Of those that a mesh axis runs over, the one named last changes fastest.
The devices are a block of a 4x16x16 slice.
Arguments:
- new_q: bfloat16 [16384, 8192], P(('rep', 'grp', 'sub'), 'tp'), parts along dimension 0
- new_kv: bfloat16 [2, 16384, 1024], P(None, ('rep', 'grp', 'sub'), 'tp'), parts along dimension 1
- hist_kv: bfloat16 [2, 32, 16, 1, 128, 1024], P(None, ('rep', 'grp'), None, None, 'sub', 'tp'), parts along dimension 1, may hold values from -6 to 6
- page_place: int32 [32, 16], P(('rep', 'grp')), parts along dimension 0, may hold values from 0 to 15, each once within a row
- hist_len: int32 [32], P(('rep', 'grp')), parts along dimension 0, may hold values from 1 to 2048, 16384 in all
- new_len: int32 [32], P(('rep', 'grp')), parts along dimension 0, may hold values from 128 to 512, as said below
- dec_q: bfloat16 [512, 8192], P(('rep', 'grp', 'sub'), 'tp'), parts along dimension 0
- dec_cache: bfloat16 [2, 512, 512, 1024], P(None, ('rep', 'grp', 'sub'), None, 'tp'), parts along dimension 1
- dec_len: int32 [512], P(('rep', 'grp', 'sub')), parts along dimension 0, may hold values from 64 to 512, as said below
Outputs:
- prefill_out: bfloat16 [16384, 8192], P(('rep', 'grp', 'sub'), 'tp'), parts along dimension 0
- decode_out: bfloat16 [512, 8192], P(('rep', 'grp', 'sub'), 'tp'), parts along dimension 0
The draws below stay inside these ranges and needn't reach their ends.
There are 2 independent parts, one for each index of `rep`. The reference program is written for one: setup_inputs(seed, part) draws one part's arguments, and reference() takes and returns one part's arrays. A program takes and returns all parts, laid end to end along the dimension named above; each array names one. Nothing has to cross between parts.
Inputs may be any that keep to these rules, and one draw needn't show every extreme that they name: `page_place`: each row is an ordering of the slots 0 to 15: each owner holds exactly 1 pages of every conversation. `hist_len`: some conversation has exactly 2048. `new_len`: some conversation has exactly 512. `dec_len`: some request has exactly 512.
All inputs are finite; a program needn't handle non-finite values. No bound on the sum of `hist_len` on one device may be relied on, other than what follows from the above.
Results may differ from the reference program's by a relative error of at most 0.008.
Values may be sent and summed in bfloat16 or wider, within the bound.
A program may use at most 128 MiB of HBM per device.

```python
import math
import jax
import jax.numpy as jnp
import numpy as np
from jax import lax

HQ = 64
KVH = 8
HD = 128
NEW = 512
PAGE = 128
P_MAX = 16
CACHE = 512
NG = 16
CAP = 1
HIST_MAX = 2048
DEC_REQ = 256


def fresh_keys(key):
    base = jax.random.normal(jax.random.fold_in(key, 11), (NG * NEW, KVH * HD), jnp.float32)
    return base


def cache_keys(key):
    base = jax.random.normal(jax.random.fold_in(key, 31), (DEC_REQ, CACHE, KVH * HD), jnp.float32)
    return base


def draw_values(key, shape):
    return jax.random.normal(key, shape, jnp.float32)


def draw_new_kv(key, part):
    keys = fresh_keys(key)
    values = draw_values(jax.random.fold_in(key, 13), keys.shape)
    return jnp.stack([keys, values]).astype(jnp.bfloat16)


def draw_new_q(key, part):
    base = jax.random.normal(jax.random.fold_in(key, 21), (NG * NEW, HQ, HD), jnp.float32)
    return base.reshape(NG * NEW, HQ * HD).astype(jnp.bfloat16)


def draw_dec_cache(key, part):
    keys = cache_keys(key)
    values = draw_values(jax.random.fold_in(key, 33), keys.shape)
    return jnp.stack([keys, values]).astype(jnp.bfloat16)


def draw_dec_q(key, part):
    base = jax.random.normal(jax.random.fold_in(key, 41), (DEC_REQ, HQ, HD), jnp.float32)
    return base.reshape(DEC_REQ, HQ * HD).astype(jnp.bfloat16)


def draw_new_len(key, part):
    counts = jax.random.randint(jax.random.fold_in(key, 51), (NG,), NEW // 4, NEW + 1)
    chosen = jax.random.randint(jax.random.fold_in(key, 52), (), 0, NG)
    return jnp.where(jnp.arange(NG) == chosen, NEW, counts).astype(jnp.int32)


def draw_dec_len(key, part):
    counts = jax.random.randint(jax.random.fold_in(key, 61), (DEC_REQ,), CACHE // 8, CACHE + 1)
    chosen = jax.random.randint(jax.random.fold_in(key, 62), (), 0, DEC_REQ)
    return jnp.where(jnp.arange(DEC_REQ) == chosen, CACHE, counts).astype(jnp.int32)


def shard_levels(key, shape, split, smallest, largest):
    def one(position, blocks):
        heights = jax.random.uniform(jax.random.fold_in(jax.random.fold_in(key, 6), position), (blocks,), jnp.float32, smallest / len(split), largest / len(split))
        return jnp.repeat(jnp.exp(heights), shape[position] // blocks).reshape((-1,) + (1,) * (len(shape) - position - 1))

    factor_of = one(*split[0])
    for cut in split[1:]:
        factor_of = factor_of * one(*cut)
    return factor_of


def length_profile(amount, total, most, slope):
    loads = [(1 << 20) // math.isqrt(rank ** slope) + 1 for rank in range(2, amount + 1)]
    surplus, given = total - most - (amount - 1), [1] * (amount - 1)
    while surplus > 0:
        candidates = [i for i in range(amount - 1) if given[i] < most]
        pool, remaining = sum([loads[i] for i in candidates]), surplus
        for i in candidates:
            addition = min(most - given[i], max(1, remaining * loads[i] // pool), surplus)
            given[i] = given[i] + addition
            surplus = surplus - addition
    return np.array([most] + given)


def ragged(stream_key, amount, total, bound, lean):
    if amount == 2:
        one = jax.random.randint(stream_key, (), max(1, total - bound), min(bound, total - 1) + 1)
        return jnp.stack([one, total - one])
    tallies = jnp.asarray(length_profile(amount, total, bound, lean), jnp.int32)
    pairs = (amount - 1) // 2
    donor, taker = tallies[1:1 + 2 * pairs:2], tallies[2:2 + 2 * pairs:2]
    slack = jnp.minimum(donor - 1, bound - taker)
    shifted = jax.random.randint(jax.random.fold_in(stream_key, 1), (pairs,), 0, 1 << 20) % (slack + 1)
    tallies = tallies.at[1:1 + 2 * pairs:2].set(donor - shifted).at[2:2 + 2 * pairs:2].set(taker + shifted)
    return tallies[jax.random.permutation(jax.random.fold_in(stream_key, 2), amount)]


def gaussian(stream_key, extent, scale, most, shards=(), kind=jnp.bfloat16):
    level = shard_levels(stream_key, extent, shards, -0.22, 0.18) if shards else 1.0
    drawn = jax.random.normal(stream_key, extent, jnp.float32) * scale * level
    return jnp.minimum(jnp.maximum(drawn, -most), most).astype(kind)


def setup_inputs(seed: int = 0, part: int = 0) -> dict:
    splits = jax.random.split(jax.random.key(seed), 10)
    part_splits = jax.random.split(jax.random.fold_in(splits[9], part), 10)
    new_q = draw_new_q(jax.random.fold_in(jax.random.fold_in(splits[9], part), 71), part)
    new_kv = draw_new_kv(jax.random.fold_in(jax.random.fold_in(splits[9], part), 71), part)
    hist_kv = gaussian(part_splits[2], (2, NG, NG, CAP, PAGE, KVH * HD), 1.0, 6.0, ((1, 16), (4, 2), (5, 4)))
    page_place = jax.vmap(lambda own: jax.random.permutation(own, P_MAX))(jax.random.split(part_splits[3], NG)).reshape((NG, P_MAX)).astype(jnp.int32)
    hist_len = ragged(part_splits[4], NG, NG * HIST_MAX // 2, HIST_MAX, 2).astype(jnp.int32)
    new_len = draw_new_len(jax.random.fold_in(jax.random.fold_in(splits[9], part), 71), part)
    dec_q = draw_dec_q(jax.random.fold_in(jax.random.fold_in(splits[9], part), 71), part)
    dec_cache = draw_dec_cache(jax.random.fold_in(jax.random.fold_in(splits[9], part), 71), part)
    dec_len = draw_dec_len(jax.random.fold_in(jax.random.fold_in(splits[9], part), 71), part)
    return dict(new_q=new_q, new_kv=new_kv, hist_kv=hist_kv, page_place=page_place, hist_len=hist_len, new_len=new_len, dec_q=dec_q, dec_cache=dec_cache, dec_len=dec_len)


NEG = -1e30


def weigh(scores, allowed, values_form, values):
    scores = jnp.where(allowed, scores, NEG)
    top = jnp.max(scores, axis=-1, keepdims=True)
    weights = jnp.exp(scores - top)
    total = jnp.sum(weights, axis=-1)
    rounded = lax.optimization_barrier(weights.astype(jnp.bfloat16))
    mixed = jnp.einsum(values_form, rounded.astype(jnp.float32), values.astype(jnp.float32))
    return mixed / total[..., None]


def reference(new_q, new_kv, hist_kv, page_place, hist_len, new_len, dec_q, dec_cache, dec_len):
    group = HQ // KVH
    scale = HD ** -0.5
    positions = jnp.arange(NEW, dtype=jnp.int32)
    hist_pos = jnp.arange(P_MAX * PAGE, dtype=jnp.int32)

    def one_conv(conv):
        owned = jnp.take(hist_kv, conv, axis=2).reshape(2, NG * CAP, PAGE, KVH, HD)
        place = jnp.take(page_place, conv, axis=0)
        ordered = jnp.take(owned, place, axis=1).reshape(2, P_MAX * PAGE, KVH, HD)
        fresh = lax.dynamic_slice_in_dim(new_kv, conv * NEW, NEW, 1).reshape(2, NEW, KVH, HD)
        keys = jnp.concatenate([ordered[0], fresh[0]], axis=0)
        values = jnp.concatenate([ordered[1], fresh[1]], axis=0)
        limit = jnp.take(hist_len, conv)
        count = jnp.take(new_len, conv)
        seen_hist = jnp.broadcast_to((hist_pos < limit)[None, :], (NEW, P_MAX * PAGE))
        seen_new = (positions[None, :] <= positions[:, None]) & (positions[None, :] < count)
        allowed = jnp.concatenate([seen_hist, seen_new], axis=1)
        queries = lax.dynamic_slice_in_dim(new_q, conv * NEW, NEW, 0).reshape(NEW, KVH, group, HD)
        scores = jnp.einsum('qkgd,skd->kgqs', queries.astype(jnp.float32), keys.astype(jnp.float32)) * scale
        mixed = weigh(scores, allowed[None, None], 'kgqs,skd->kgqd', values)
        out = jnp.transpose(mixed, (2, 0, 1, 3)).reshape(NEW, HQ * HD)
        out = jnp.where((positions < count)[:, None], out, 0.0)
        return out.astype(jnp.bfloat16)

    prefill_out = lax.map(one_conv, jnp.arange(NG, dtype=jnp.int32)).reshape(NG * NEW, HQ * HD)

    requests = dec_q.shape[0]
    dq = dec_q.reshape(requests, KVH, group, HD).astype(jnp.float32)
    dkeys = dec_cache[0].reshape(requests, CACHE, KVH, HD).astype(jnp.float32)
    dvalues = dec_cache[1].reshape(requests, CACHE, KVH, HD)
    dscores = jnp.einsum('rkgd,rskd->rkgs', dq, dkeys) * scale
    dallowed = (jnp.arange(CACHE, dtype=jnp.int32)[None, :] < dec_len[:, None])[:, None, None, :]
    dmixed = weigh(dscores, dallowed, 'rkgs,rskd->rkgd', dvalues)
    decode_out = dmixed.reshape(requests, HQ * HD).astype(jnp.bfloat16)
    return prefill_out, decode_out
```

```python
import math

import jax
import jax.numpy as jnp
from jax import lax
from jax.experimental import pallas as pl
from jax.experimental.pallas import tpu as pltpu
from jax.sharding import PartitionSpec as P

HD = 128
PAGE = 128
NEG = -1e30
MESH = pl.DeviceIdType.MESH
SCALE2 = (HD**-0.5) * math.log2(math.e)


def step_of(j):
    odd = j % 2
    return odd * ((j + 1) // 2) - (1 - odd) * (j // 2)


def nt(a, b):
    return lax.dot_general(a, b, (((1,), (0,)), ((), ())), preferred_element_type=jnp.float32)


def body(
    ng,
    q_hbm,
    nkv_hbm,
    hist_hbm,
    place,
    hlen,
    nlen,
    dq_hbm,
    dkv_hbm,
    dlen,
    out,
    dout,
    q_v,
    nkv,
    nkv_far,
    hist,
    dq_v,
    dkv,
    near,
    far,
    qt,
    kb,
    vt,
    bias,
    acc,
    top,
    total,
    local_sem,
    send_sem,
    recv_sem,
    fsend_sem,
    frecv_sem,
):
    z = lax.axis_index("grp")
    sub = lax.axis_index("sub")
    heads = qt.shape[0]
    kvh = kb.shape[0]
    group = heads // kvh
    rows = q_v.shape[0]
    half = near.shape[2]
    reqs, cached = dkv.shape[1], dkv.shape[2]

    barrier = pltpu.get_barrier_semaphore()
    for k in range(1, ng):
        pl.semaphore_signal(
            barrier, inc=1, device_id={"grp": (z + k) % ng}, device_id_type=MESH
        )
    pl.semaphore_signal(barrier, inc=1, device_id={"sub": 1 - sub}, device_id_type=MESH)

    load_hist = pltpu.make_async_copy(hist_hbm.at[:, 0, :, 0], hist, local_sem.at[0])
    load_own = pltpu.make_async_copy(hist_hbm.at[:, 0, z, 0], near.at[0], local_sem.at[1])
    load_nkv = pltpu.make_async_copy(nkv_hbm, nkv, local_sem.at[2])
    load_q = pltpu.make_async_copy(q_hbm, q_v, local_sem.at[3])
    load_dq = pltpu.make_async_copy(dq_hbm, dq_v, local_sem.at[4])
    load_dkv = pltpu.make_async_copy(dkv_hbm, dkv, local_sem.at[5])
    for load in (load_hist, load_own, load_nkv, load_q, load_dq, load_dkv):
        load.start()
    load_hist.wait()
    load_own.wait()
    load_nkv.wait()
    pl.semaphore_wait(barrier, ng)

    sends = []
    for j in range(1, ng):
        k = step_of(j)
        sends.append(
            pltpu.make_async_remote_copy(
                src_ref=hist.at[:, (z + k + ng) % ng],
                dst_ref=near.at[j],
                send_sem=send_sem.at[j],
                recv_sem=recv_sem.at[j],
                device_id={"grp": (z + k + ng) % ng},
                device_id_type=MESH,
            )
        )
        sends[-1].start()

    def forward(j):
        return pltpu.make_async_remote_copy(
            src_ref=near.at[j],
            dst_ref=far.at[j],
            send_sem=fsend_sem.at[j],
            recv_sem=frecv_sem.at[j],
            device_id={"sub": 1 - sub},
            device_id_type=MESH,
        )

    def arrival(j):
        return pltpu.make_async_remote_copy(
            src_ref=near.at[j],
            dst_ref=near.at[j],
            send_sem=send_sem.at[j],
            recv_sem=recv_sem.at[j],
            device_id={"grp": (z + 1) % ng},
            device_id_type=MESH,
        )

    swap = pltpu.make_async_remote_copy(
        src_ref=nkv,
        dst_ref=nkv_far,
        send_sem=fsend_sem.at[ng],
        recv_sem=frecv_sem.at[ng],
        device_id={"sub": 1 - sub},
        device_id_type=MESH,
    )
    swap.start()
    forward(0).start()

    load_q.wait()
    for h in range(heads):
        qt[h] = q_v[:, h * HD : (h + 1) * HD].astype(jnp.float32).T.astype(jnp.bfloat16)
    top[...] = jnp.full_like(top, NEG)
    total[...] = jnp.zeros_like(total)
    acc[...] = jnp.zeros_like(acc)

    def set_keys(keys, values):
        for g in range(kvh):
            lanes = slice(g * HD, (g + 1) * HD)
            kb[g] = jnp.concatenate([r[:, lanes] for r in keys], axis=0)
            v = jnp.concatenate([r[:, lanes] for r in values], axis=0)
            vt[g] = v.astype(jnp.float32).T.astype(jnp.bfloat16)

    def attend():
        def one(g, carry):
            k = kb[g]
            v = vt[g]
            for i in range(group):
                h = g * group + i
                s = nt(k, qt[h]) + bias[...]
                old = top[h]
                new = jnp.maximum(old, jnp.max(s, axis=0, keepdims=True))
                w = jnp.exp2((s - new) * SCALE2)
                fade = jnp.exp2((old - new) * SCALE2)
                top[h] = new
                total[h] = total[h] * fade + jnp.sum(w, axis=0, keepdims=True)
                acc[h] = acc[h] * fade + nt(v, w.astype(jnp.bfloat16))
            return carry

        lax.fori_loop(0, kvh, one, 0)

    count = nlen[0]
    square = bias.shape
    key_row = lax.broadcasted_iota(jnp.int32, square, 0)
    query_row = lax.broadcasted_iota(jnp.int32, square, 1)

    seen = (key_row <= query_row) & (sub * rows + key_row < count)
    bias[...] = jnp.where(seen, 0.0, NEG)
    set_keys([nkv.at[0]], [nkv.at[1]])
    attend()

    load_dq.wait()
    load_dkv.wait()
    dq = dq_v[...].astype(jnp.float32)
    wide = heads * reqs
    dq_rows = jnp.concatenate([dq[:, h * HD : (h + 1) * HD] for h in range(heads)], axis=0)
    dq_cols = dq_rows.T
    col = lax.broadcasted_iota(jnp.int32, (HD, wide), 1)
    col_req = col % reqs
    col_kv = col // (reqs * group)
    ds = None
    for r in range(reqs):
        blocks = [
            jnp.where((col_req == r) & (col_kv == g), dq_cols, 0.0).astype(jnp.bfloat16)
            for g in range(kvh)
        ]
        term = nt(dkv[0, r], jnp.concatenate(blocks, axis=0))
        ds = term if ds is None else ds + term
    limit_row = jnp.zeros((1, wide), jnp.int32)
    req_row = lax.broadcasted_iota(jnp.int32, (1, wide), 1) % reqs
    for r in range(reqs):
        limit_row = jnp.where(req_row == r, dlen[r], limit_row)
    dpos = lax.broadcasted_iota(jnp.int32, (cached, wide), 0)
    ds = jnp.where(dpos < limit_row, ds, NEG)
    dw = jnp.exp2((ds - jnp.max(ds, axis=0, keepdims=True)) * SCALE2)
    dwt = dw.T
    dtotal = jnp.sum(dwt, axis=1, keepdims=True)
    dwt = dwt.astype(jnp.bfloat16)
    row_req = lax.broadcasted_iota(jnp.int32, (wide, HD), 0) % reqs
    part = group * reqs
    dmix = jnp.zeros((wide, HD), jnp.float32)
    for r in range(reqs):
        full = nt(dwt, dkv[1, r])
        picked = jnp.concatenate(
            [full[g * part : (g + 1) * part, g * HD : (g + 1) * HD] for g in range(kvh)], axis=0
        )
        dmix = jnp.where(row_req == r, picked, dmix)
    dmix = dmix / dtotal
    for h in range(heads):
        dout[:, h * HD : (h + 1) * HD] = dmix[h * reqs : (h + 1) * reqs].astype(jnp.bfloat16)

    swap.wait_recv()

    @pl.when(sub == 1)
    def _():
        bias[...] = jnp.where(key_row < count, 0.0, NEG)
        set_keys([nkv_far.at[0]], [nkv_far.at[1]])
        attend()

    limit = hlen[0]
    token = lax.broadcasted_iota(jnp.int32, (half, square[1]), 0)

    def page_of(j):
        owner = (z - step_of(j) + ng) % ng
        page = 0
        for p in range(ng):
            page = page + jnp.where(place[0, p] == owner, p, 0)
        return page

    def pair(b, carry):
        for j in (2 * b, 2 * b + 1):

            @pl.when(j > 0)
            def _():
                arrival(j).wait_recv()
                forward(j).start()

        for i in range(2):
            j = 2 * b + i
            start = page_of(j) * PAGE
            for n, who in enumerate((sub, 1 - sub)):
                position = start + who * half + token
                at = (2 * i + n) * half
                bias[at : at + half] = jnp.where(position < limit, 0.0, NEG)
        for j in (2 * b, 2 * b + 1):
            forward(j).wait_recv()
        parts = [r.at[j] for j in (2 * b, 2 * b + 1) for r in (near, far)]
        set_keys([p.at[0] for p in parts], [p.at[1] for p in parts])
        attend()
        return carry

    lax.fori_loop(0, ng // 2, pair, 0)

    kept = sub * rows + lax.broadcasted_iota(jnp.int32, (1, rows), 1) < count
    for h in range(heads):
        mixed = jnp.where(kept, acc[h] / total[h], 0.0)
        out[:, h * HD : (h + 1) * HD] = mixed.T.astype(jnp.bfloat16)

    for send in sends:
        send.wait_send()
    swap.wait_send()
    for j in range(ng):
        forward(j).wait_send()


def solution(mesh):
    ng = mesh.shape["grp"]

    def shards(new_q, new_kv, hist_kv, page_place, hist_len, new_len, dec_q, dec_cache, dec_len):
        rows, width = new_q.shape
        heads = width // HD
        kvh = new_kv.shape[2] // HD
        half, lanes = hist_kv.shape[4:]
        keys = 4 * half
        anywhere = pl.BlockSpec(memory_space=pl.ANY)
        scalars = pl.BlockSpec(memory_space=pltpu.SMEM)
        vmem = pl.BlockSpec(memory_space=pltpu.VMEM)
        bf16, f32 = jnp.bfloat16, jnp.float32

        def kernel(*refs):
            body(ng, *refs)

        return pl.pallas_call(
            kernel,
            name="serve",
            out_shape=(
                jax.ShapeDtypeStruct(new_q.shape, bf16),
                jax.ShapeDtypeStruct(dec_q.shape, bf16),
            ),
            in_specs=[anywhere] * 3 + [scalars] * 3 + [anywhere] * 2 + [scalars],
            out_specs=(vmem, vmem),
            scratch_shapes=[
                pltpu.VMEM(new_q.shape, bf16),
                pltpu.VMEM(new_kv.shape, bf16),
                pltpu.VMEM(new_kv.shape, bf16),
                pltpu.VMEM((2, ng, half, lanes), bf16),
                pltpu.VMEM(dec_q.shape, bf16),
                pltpu.VMEM(dec_cache.shape, bf16),
                pltpu.VMEM((ng, 2, half, lanes), bf16),
                pltpu.VMEM((ng, 2, half, lanes), bf16),
                pltpu.VMEM((heads, HD, rows), bf16),
                pltpu.VMEM((kvh, keys, HD), bf16),
                pltpu.VMEM((kvh, HD, keys), bf16),
                pltpu.VMEM((keys, rows), f32),
                pltpu.VMEM((heads, HD, rows), f32),
                pltpu.VMEM((heads, 1, rows), f32),
                pltpu.VMEM((heads, 1, rows), f32),
                pltpu.SemaphoreType.DMA((6,)),
                pltpu.SemaphoreType.DMA((ng,)),
                pltpu.SemaphoreType.DMA((ng,)),
                pltpu.SemaphoreType.DMA((ng + 1,)),
                pltpu.SemaphoreType.DMA((ng + 1,)),
            ],
            compiler_params=pltpu.CompilerParams(
                collective_id=0, has_side_effects=True, vmem_limit_bytes=48 * 1024 * 1024
            ),
        )(new_q, new_kv, hist_kv, page_place, hist_len, new_len, dec_q, dec_cache, dec_len)

    in_specs = (
        P(("rep", "grp", "sub"), "tp"),
        P(None, ("rep", "grp", "sub"), "tp"),
        P(None, ("rep", "grp"), None, None, "sub", "tp"),
        P(("rep", "grp"), None),
        P(("rep", "grp")),
        P(("rep", "grp")),
        P(("rep", "grp", "sub"), "tp"),
        P(None, ("rep", "grp", "sub"), None, "tp"),
        P(("rep", "grp", "sub")),
    )
    out_specs = (P(("rep", "grp", "sub"), "tp"), P(("rep", "grp", "sub"), "tp"))
    return jax.shard_map(shards, mesh=mesh, in_specs=in_specs, out_specs=out_specs, check_vma=False)
```

```python
import math

import jax
import jax.numpy as jnp
from jax import lax
from jax.experimental import pallas as pl
from jax.experimental.pallas import tpu as pltpu
from jax.sharding import PartitionSpec as P

HD = 128
PAGE = 128
NEG = -1e30
MESH = pl.DeviceIdType.MESH
SCALE2 = (HD**-0.5) * math.log2(math.e)


def step_of(j):
    odd = j % 2
    return odd * ((j + 1) // 2) - (1 - odd) * (j // 2)


def nt(a, b):
    return lax.dot_general(a, b, (((1,), (0,)), ((), ())), preferred_element_type=jnp.float32)


def body(
    ng,
    q_hbm,
    nkv_hbm,
    hist_hbm,
    place_hbm,
    hlen,
    nlen,
    dq_hbm,
    dkv_hbm,
    dlen_hbm,
    out,
    dout,
    q_v,
    nkv,
    nkv_far,
    hist,
    dq_v,
    dkv,
    near,
    far,
    qt,
    kb,
    vt,
    acc,
    top,
    total,
    place,
    dlen,
    local_sem,
    send_sem,
    recv_sem,
    fsend_sem,
    frecv_sem,
):
    z = lax.axis_index("grp")
    sub = lax.axis_index("sub")
    heads = qt.shape[0]
    kvh = kb.shape[0]
    group = heads // kvh
    rows = q_v.shape[0]
    half = near.shape[2]
    reqs, cached = dkv.shape[1], dkv.shape[2]

    barrier = pltpu.get_barrier_semaphore()
    for k in range(1, ng):
        pl.semaphore_signal(
            barrier, inc=1, device_id={"grp": (z + k) % ng}, device_id_type=MESH
        )
    pl.semaphore_signal(barrier, inc=1, device_id={"sub": 1 - sub}, device_id_type=MESH)

    load_hist = pltpu.make_async_copy(hist_hbm.at[:, 0, :, 0], hist, local_sem.at[0])
    load_own = pltpu.make_async_copy(hist_hbm.at[:, 0, z, 0], near.at[0], local_sem.at[1])
    load_nkv = pltpu.make_async_copy(nkv_hbm, nkv, local_sem.at[2])
    load_q = pltpu.make_async_copy(q_hbm, q_v, local_sem.at[3])
    load_dq = pltpu.make_async_copy(dq_hbm, dq_v, local_sem.at[4])
    load_dkv = pltpu.make_async_copy(dkv_hbm, dkv, local_sem.at[5])
    load_scalars = [
        pltpu.make_async_copy(place_hbm, place, local_sem.at[6]),
        pltpu.make_async_copy(dlen_hbm, dlen, local_sem.at[7]),
    ]
    for load in (load_hist, load_own, load_nkv, load_q, load_dq, *load_scalars, load_dkv):
        load.start()
    load_hist.wait()
    load_own.wait()
    load_nkv.wait()
    pl.semaphore_wait(barrier, ng)

    sends = []
    for j in range(1, ng):
        k = step_of(j)
        sends.append(
            pltpu.make_async_remote_copy(
                src_ref=hist.at[:, (z + k + ng) % ng],
                dst_ref=near.at[j],
                send_sem=send_sem.at[j],
                recv_sem=recv_sem.at[j],
                device_id={"grp": (z + k + ng) % ng},
                device_id_type=MESH,
            )
        )
        sends[-1].start()

    def forward(j):
        return pltpu.make_async_remote_copy(
            src_ref=near.at[j],
            dst_ref=far.at[j],
            send_sem=fsend_sem.at[j],
            recv_sem=frecv_sem.at[j],
            device_id={"sub": 1 - sub},
            device_id_type=MESH,
        )

    def arrival(j):
        return pltpu.make_async_remote_copy(
            src_ref=near.at[j],
            dst_ref=near.at[j],
            send_sem=send_sem.at[j],
            recv_sem=recv_sem.at[j],
            device_id={"grp": (z + 1) % ng},
            device_id_type=MESH,
        )

    swap = pltpu.make_async_remote_copy(
        src_ref=nkv,
        dst_ref=nkv_far,
        send_sem=fsend_sem.at[ng],
        recv_sem=frecv_sem.at[ng],
        device_id={"sub": 1 - sub},
        device_id_type=MESH,
    )
    swap.start()
    forward(0).start()

    load_q.wait()
    for load in load_scalars:
        load.wait()
    one_row = (lax.broadcasted_iota(jnp.int32, (HD, rows), 0) == 0).astype(jnp.float32)
    one_row = one_row.astype(jnp.bfloat16)
    for h in range(heads):
        scaled = q_v[:, h * HD : (h + 1) * HD].astype(jnp.float32) * SCALE2
        qt[h, :HD] = scaled.T.astype(jnp.bfloat16)
        qt[h, HD:] = one_row
    top[...] = jnp.full_like(top, NEG)
    total[...] = jnp.zeros_like(total)
    acc[...] = jnp.zeros_like(acc)

    def set_keys(keys, values, biases):
        for g in range(kvh):
            lanes = slice(g * HD, (g + 1) * HD)
            kb[g, :, :HD] = jnp.concatenate([r[:, lanes] for r in keys], axis=0)
            kb[g, :, HD:] = jnp.concatenate(biases, axis=0)
            v = jnp.concatenate([r[:, lanes] for r in values], axis=0)
            vt[g] = v.astype(jnp.float32).T.astype(jnp.bfloat16)

    span = kb.shape[1]

    def attend(causal):
        def score(h):
            s = nt(kb[h // group], qt[h])
            if causal:
                key = lax.broadcasted_iota(jnp.int32, s.shape, 0)
                query = lax.broadcasted_iota(jnp.int32, s.shape, 1)
                s = jnp.where(key <= query, s, NEG)
            return s.reshape(span // 8, 8, rows)

        def weigh(h, s):
            old = top[h]
            new = jnp.maximum(old, jnp.max(s, axis=0))
            for shift in (4, 2, 1):
                new = jnp.maximum(new, pltpu.roll(new, shift, 0))
            fade = jnp.exp2(old - new)
            w = jnp.exp2(s - new[None])
            top[h] = new
            total[h] = total[h] * fade + jnp.sum(w, axis=0)
            return w.reshape(span, rows).astype(jnp.bfloat16), fade

        def mix(h, w, fade):
            kept = acc[h].reshape(HD // 8, 8, rows) * fade[None]
            acc[h] = kept.reshape(HD, rows) + nt(vt[h // group], w)

        s = score(0)
        last = None
        for h in range(heads):
            ahead = score(h + 1) if h + 1 < heads else None
            w, fade = weigh(h, s)
            if last is not None:
                mix(*last)
            last = (h, w, fade)
            s = ahead
        mix(*last)

    count = nlen[0]

    def hide(shape, start, limit):
        position = start + lax.broadcasted_iota(jnp.int32, shape, 0)
        return jnp.where(position < limit, 0.0, NEG).astype(jnp.bfloat16)

    set_keys([nkv.at[0]], [nkv.at[1]], [hide((rows, HD), sub * rows, count)])
    attend(True)

    load_dq.wait()
    load_dkv.wait()
    dq = dq_v[...].astype(jnp.float32)
    wide = heads * reqs
    dq_rows = jnp.concatenate([dq[:, h * HD : (h + 1) * HD] for h in range(heads)], axis=0)
    dq_cols = dq_rows.T
    col = lax.broadcasted_iota(jnp.int32, (HD, wide), 1)
    col_req = col % reqs
    col_kv = col // (reqs * group)
    ds = None
    for r in range(reqs):
        blocks = [
            jnp.where((col_req == r) & (col_kv == g), dq_cols, 0.0).astype(jnp.bfloat16)
            for g in range(kvh)
        ]
        term = nt(dkv[0, r], jnp.concatenate(blocks, axis=0))
        ds = term if ds is None else ds + term
    limit_row = jnp.zeros((1, wide), jnp.int32)
    req_row = lax.broadcasted_iota(jnp.int32, (1, wide), 1) % reqs
    for r in range(reqs):
        limit_row = jnp.where(req_row == r, dlen[r], limit_row)
    dpos = lax.broadcasted_iota(jnp.int32, (cached, wide), 0)
    ds = jnp.where(dpos < limit_row, ds, NEG)
    dw = jnp.exp2((ds - jnp.max(ds, axis=0, keepdims=True)) * SCALE2)
    dwt = dw.T
    dtotal = jnp.sum(dwt, axis=1, keepdims=True)
    dwt = dwt.astype(jnp.bfloat16)
    row_req = lax.broadcasted_iota(jnp.int32, (wide, HD), 0) % reqs
    part = group * reqs
    dmix = jnp.zeros((wide, HD), jnp.float32)
    for r in range(reqs):
        full = nt(dwt, dkv[1, r])
        picked = jnp.concatenate(
            [full[g * part : (g + 1) * part, g * HD : (g + 1) * HD] for g in range(kvh)], axis=0
        )
        dmix = jnp.where(row_req == r, picked, dmix)
    dmix = dmix / dtotal
    for h in range(heads):
        dout[:, h * HD : (h + 1) * HD] = dmix[h * reqs : (h + 1) * reqs].astype(jnp.bfloat16)

    swap.wait_recv()

    @pl.when(sub == 1)
    def _():
        set_keys([nkv_far.at[0]], [nkv_far.at[1]], [hide((rows, HD), 0, count)])
        attend(False)

    limit = hlen[0]

    def page_of(j):
        owner = (z - step_of(j) + ng) % ng
        page = 0
        for p in range(ng):
            page = page + jnp.where(place[0, p] == owner, p, 0)
        return page

    def take(b):
        for j in (2 * b, 2 * b + 1):
            arrival(j).wait_recv()
            forward(j).start()

    def use(b):
        slots = (2 * b, 2 * b + 1)
        biases = [
            hide((half, HD), page_of(j) * PAGE + who * half, limit)
            for j in slots
            for who in (sub, 1 - sub)
        ]
        for j in slots:
            forward(j).wait_recv()
        parts = [r.at[j] for j in slots for r in (near, far)]
        set_keys([p.at[0] for p in parts], [p.at[1] for p in parts], biases)
        attend(False)

    arrival(1).wait_recv()
    forward(1).start()
    pairs = ng // 2

    def pair(b, carry):
        @pl.when(b < pairs - 1)
        def _():
            take(b)

        use(b - 1)

        @pl.when(b == pairs - 1)
        def _():
            take(b)

        return carry

    lax.fori_loop(1, pairs, pair, 0)
    use(pairs - 1)

    kept = sub * rows + lax.broadcasted_iota(jnp.int32, (1, rows), 1) < count
    for h in range(heads):
        mixed = jnp.where(kept, acc[h] / jnp.sum(total[h], axis=0, keepdims=True), 0.0)
        out[:, h * HD : (h + 1) * HD] = mixed.T.astype(jnp.bfloat16)

    for send in sends:
        send.wait_send()
    swap.wait_send()
    for j in range(ng):
        forward(j).wait_send()


def solution(mesh):
    ng = mesh.shape["grp"]

    def shards(new_q, new_kv, hist_kv, page_place, hist_len, new_len, dec_q, dec_cache, dec_len):
        rows, width = new_q.shape
        heads = width // HD
        kvh = new_kv.shape[2] // HD
        half, lanes = hist_kv.shape[4:]
        keys = 4 * half
        anywhere = pl.BlockSpec(memory_space=pltpu.HBM)
        scalars = pl.BlockSpec(memory_space=pltpu.SMEM)
        vmem = pl.BlockSpec(memory_space=pltpu.VMEM)
        bf16, f32 = jnp.bfloat16, jnp.float32

        def keep(x):
            return pltpu.with_memory_space_constraint(x, pltpu.HBM)

        def kernel(*refs):
            body(ng, *refs)

        return pl.pallas_call(
            kernel,
            name="serve",
            out_shape=(
                jax.ShapeDtypeStruct(new_q.shape, bf16),
                jax.ShapeDtypeStruct(dec_q.shape, bf16),
            ),
            in_specs=[anywhere] * 4 + [scalars] * 2 + [anywhere] * 3,
            out_specs=(vmem, vmem),
            scratch_shapes=[
                pltpu.VMEM(new_q.shape, bf16),
                pltpu.VMEM(new_kv.shape, bf16),
                pltpu.VMEM(new_kv.shape, bf16),
                pltpu.VMEM((2, ng, half, lanes), bf16),
                pltpu.VMEM(dec_q.shape, bf16),
                pltpu.VMEM(dec_cache.shape, bf16),
                pltpu.VMEM((ng, 2, half, lanes), bf16),
                pltpu.VMEM((ng, 2, half, lanes), bf16),
                pltpu.VMEM((heads, 2 * HD, rows), bf16),
                pltpu.VMEM((kvh, keys, 2 * HD), bf16),
                pltpu.VMEM((kvh, HD, keys), bf16),
                pltpu.VMEM((heads, HD, rows), f32),
                pltpu.VMEM((heads, 8, rows), f32),
                pltpu.VMEM((heads, 8, rows), f32),
                pltpu.SMEM(page_place.shape, jnp.int32),
                pltpu.SMEM(dec_len.shape, jnp.int32),
                pltpu.SemaphoreType.DMA((8,)),
                pltpu.SemaphoreType.DMA((ng,)),
                pltpu.SemaphoreType.DMA((ng,)),
                pltpu.SemaphoreType.DMA((ng + 1,)),
                pltpu.SemaphoreType.DMA((ng + 1,)),
            ],
            compiler_params=pltpu.CompilerParams(
                collective_id=0, has_side_effects=True, vmem_limit_bytes=40 * 1024 * 1024
            ),
        )(
            *(keep(x) for x in (new_q, new_kv, hist_kv, page_place)),
            hist_len,
            new_len,
            *(keep(x) for x in (dec_q, dec_cache, dec_len)),
        )

    in_specs = (
        P(("rep", "grp", "sub"), "tp"),
        P(None, ("rep", "grp", "sub"), "tp"),
        P(None, ("rep", "grp"), None, None, "sub", "tp"),
        P(("rep", "grp"), None),
        P(("rep", "grp")),
        P(("rep", "grp")),
        P(("rep", "grp", "sub"), "tp"),
        P(None, ("rep", "grp", "sub"), None, "tp"),
        P(("rep", "grp", "sub")),
    )
    out_specs = (P(("rep", "grp", "sub"), "tp"), P(("rep", "grp", "sub"), "tp"))
    return jax.shard_map(shards, mesh=mesh, in_specs=in_specs, out_specs=out_specs, check_vma=False)
```

```python
import math

import jax
import jax.numpy as jnp
from jax import lax
from jax.experimental import pallas as pl
from jax.experimental.pallas import tpu as pltpu
from jax.sharding import PartitionSpec as P

HD = 128
PAGE = 128
NEG = -1e30
MESH = pl.DeviceIdType.MESH
SCALE2 = (HD**-0.5) * math.log2(math.e)


def source_of(j, z, ng):
    odd = j % 2
    step = odd * ((j + 1) // 2) - (1 - odd) * (j // 2)
    return (z + step + ng) % ng


def nt(a, b):
    return lax.dot_general(a, b, (((1,), (0,)), ((), ())), preferred_element_type=jnp.float32)


def body(
    ng,
    q_hbm,
    nkv_hbm,
    hist_hbm,
    place_hbm,
    hlen,
    nlen,
    dq_hbm,
    dkv_hbm,
    dlen_hbm,
    out,
    dout,
    q_v,
    nkv,
    nkv_far,
    hist,
    dq_v,
    dkv,
    near,
    far,
    qt,
    kb,
    vt,
    acc,
    top,
    total,
    place,
    dlen,
    local_sem,
    send_sem,
    recv_sem,
    fsend_sem,
    frecv_sem,
    in_sem,
):
    z = lax.axis_index("grp")
    sub = lax.axis_index("sub")
    heads = qt.shape[0]
    kvh = kb.shape[0]
    group = heads // kvh
    rows = q_v.shape[0]
    half = near.shape[2]
    reqs, cached = dkv.shape[1], dkv.shape[2]

    low = ng // 2
    early = low - 3
    first = jnp.where(lax.axis_index("tp") == 0, ng - 2, low)
    barrier = pltpu.get_barrier_semaphore()

    def greet(d):
        pl.semaphore_signal(barrier, inc=1, device_id={"grp": d}, device_id_type=MESH)

    def tell(sem, d):
        pl.semaphore_signal(sem, inc=1, device_id={"grp": d}, device_id_type=MESH)

    pl.semaphore_signal(barrier, inc=1, device_id={"sub": 1 - sub}, device_id_type=MESH)

    for d in range(low, ng):

        @pl.when((z == 0) & ((first == low) | (first == d)))
        def _():
            greet(d)

    load_hist = pltpu.make_async_copy(hist_hbm.at[:, 0, :, 0], hist, local_sem.at[0])
    load_own = pltpu.make_async_copy(hist_hbm.at[:, 0, z, 0], near.at[z], local_sem.at[1])
    load_nkv = pltpu.make_async_copy(nkv_hbm, nkv, local_sem.at[2])
    load_q = pltpu.make_async_copy(q_hbm, q_v, local_sem.at[3])
    load_dq = pltpu.make_async_copy(dq_hbm, dq_v, local_sem.at[4])
    load_dkv = pltpu.make_async_copy(dkv_hbm, dkv, local_sem.at[5])
    load_scalars = [
        pltpu.make_async_copy(place_hbm, place, local_sem.at[6]),
        pltpu.make_async_copy(dlen_hbm, dlen, local_sem.at[7]),
    ]
    for load in (load_hist, load_own, load_nkv, load_q, load_dq, *load_scalars, load_dkv):
        load.start()
    load_hist.wait()
    load_own.wait()
    load_nkv.wait()
    pred = jnp.where(z >= 2, 1, 0)
    zero = jnp.where(((first == low) & (z >= low)) | (first == z), 1, 0)
    pl.semaphore_wait(barrier, 1 + pred + zero)

    def send(d):
        return pltpu.make_async_remote_copy(
            src_ref=hist.at[:, d],
            dst_ref=near.at[z],
            send_sem=send_sem.at[d],
            recv_sem=recv_sem.at[z],
            device_id={"grp": d},
            device_id_type=MESH,
        )

    @pl.when((z >= 1) & (z < ng - 1))
    def _():
        greet(z + 1)

    for d in range(ng - 1):

        @pl.when(z >= first if d == 0 else z > d)
        def _():
            tell(in_sem.at[z], d)

    def give(when, d):
        @pl.when(when)
        def _():
            send(d).start()

    for t in range(low):
        straight = (z >= first) | ((first == low) & (z >= low))
        give(straight & (t <= z - low), t)
        if t < low - 1:
            down = z - 1 - t
            give((z >= low) | ((z >= 1) & (down >= 1)), down)

    def hear(d):
        pl.semaphore_wait(in_sem.at[d], 1)

    def reach_up():
        for d in range(2, low):

            @pl.when((z >= 1) & (z < d))
            def _():
                hear(d)
                send(d).start()

        hear(first)
        give(z >= 1, 0)
        for t in range(1, low):
            give((z == 0) & (t < first), t)
            if low < ng - 1 - t:
                give((z == 0) & (ng - 1 - t < first), ng - 1 - t)
        give((z == 0) & (low < first), low)
        for d in range(low, ng):

            @pl.when(((z >= 1) | (d >= first)) & (d != first))
            def _():
                hear(d)

            give((z >= 1) | (d >= first), d)

    def forward(s):
        return pltpu.make_async_remote_copy(
            src_ref=near.at[s],
            dst_ref=far.at[s],
            send_sem=fsend_sem.at[s],
            recv_sem=frecv_sem.at[s],
            device_id={"sub": 1 - sub},
            device_id_type=MESH,
        )

    def arrival(s):
        return pltpu.make_async_remote_copy(
            src_ref=near.at[s],
            dst_ref=near.at[s],
            send_sem=send_sem.at[s],
            recv_sem=recv_sem.at[s],
            device_id={"sub": 1 - sub},
            device_id_type=MESH,
        )

    swap = pltpu.make_async_remote_copy(
        src_ref=nkv,
        dst_ref=nkv_far,
        send_sem=fsend_sem.at[ng],
        recv_sem=frecv_sem.at[ng],
        device_id={"sub": 1 - sub},
        device_id_type=MESH,
    )
    swap.start()
    forward(z).start()

    @pl.when(z >= low)
    def _():
        @pl.when((first != low) & (z < first))
        def _():
            hear(first)

        for t in range(low):
            give((first != low) & (z < first) & (t <= z - low), t)
        for d in range(low + 1, ng):

            @pl.when((z < d) & (d != first))
            def _():
                hear(d)

            give(z < d, d)

    @pl.when((z >= early) & (z < low))
    def _():
        reach_up()


    load_q.wait()
    for load in load_scalars:
        load.wait()
    one_row = (lax.broadcasted_iota(jnp.int32, (HD, rows), 0) == 0).astype(jnp.float32)
    one_row = one_row.astype(jnp.bfloat16)
    for h in range(heads):
        scaled = q_v[:, h * HD : (h + 1) * HD].astype(jnp.float32) * SCALE2
        qt[h, :HD] = scaled.T.astype(jnp.bfloat16)
        qt[h, HD:] = one_row
    top[...] = jnp.full_like(top, NEG)
    total[...] = jnp.zeros_like(total)
    acc[...] = jnp.zeros_like(acc)

    def set_keys(keys, values, biases):
        for g in range(kvh):
            lanes = slice(g * HD, (g + 1) * HD)
            kb[g, :, :HD] = jnp.concatenate([r[:, lanes] for r in keys], axis=0)
            kb[g, :, HD:] = jnp.concatenate(biases, axis=0)
            v = jnp.concatenate([r[:, lanes] for r in values], axis=0)
            vt[g] = v.astype(jnp.float32).T.astype(jnp.bfloat16)

    span = kb.shape[1]

    def attend(causal, last_block=False):
        def score(h):
            s = nt(kb[h // group], qt[h])
            if causal:
                key = lax.broadcasted_iota(jnp.int32, s.shape, 0)
                query = lax.broadcasted_iota(jnp.int32, s.shape, 1)
                s = jnp.where(key <= query, s, NEG)
            return s.reshape(span // 8, 8, rows)

        def weigh(h, s):
            old = top[h]
            new = jnp.maximum(old, jnp.max(s, axis=0))
            for shift in (4, 2, 1):
                new = jnp.maximum(new, pltpu.roll(new, shift, 0))
            fade = jnp.exp2(old - new)
            w = jnp.exp2(s - new[None])
            top[h] = new
            total[h] = total[h] * fade + jnp.sum(w, axis=0)
            return w.reshape(span, rows).astype(jnp.bfloat16), fade

        def mix(h, w, fade):
            kept = acc[h].reshape(HD // 8, 8, rows) * fade[None]
            mixed = kept.reshape(HD, rows) + nt(vt[h // group], w)
            if last_block:
                mixed = mixed / jnp.sum(total[h], axis=0, keepdims=True)
                mixed = jnp.where(live, mixed, 0.0)
                out[:, h * HD : (h + 1) * HD] = mixed.T.astype(jnp.bfloat16)
            else:
                acc[h] = mixed

        s = score(0)
        last = None
        for h in range(heads):
            ahead = score(h + 1) if h + 1 < heads else None
            w, fade = weigh(h, s)
            if last is not None:
                mix(*last)
            last = (h, w, fade)
            s = ahead
        mix(*last)

    count = nlen[0]
    live = sub * rows + lax.broadcasted_iota(jnp.int32, (1, rows), 1) < count

    def hide(shape, start, limit):
        position = start + lax.broadcasted_iota(jnp.int32, shape, 0)
        return jnp.where(position < limit, 0.0, NEG).astype(jnp.bfloat16)

    set_keys([nkv.at[0]], [nkv.at[1]], [hide((rows, HD), sub * rows, count)])
    attend(True)

    load_dq.wait()
    load_dkv.wait()
    dq = dq_v[...].astype(jnp.float32)
    wide = heads * reqs
    dq_rows = jnp.concatenate([dq[:, h * HD : (h + 1) * HD] for h in range(heads)], axis=0)
    dq_cols = dq_rows.T
    col = lax.broadcasted_iota(jnp.int32, (HD, wide), 1)
    col_req = col % reqs
    col_kv = col // (reqs * group)
    ds = None
    for r in range(reqs):
        blocks = [
            jnp.where((col_req == r) & (col_kv == g), dq_cols, 0.0).astype(jnp.bfloat16)
            for g in range(kvh)
        ]
        term = nt(dkv[0, r], jnp.concatenate(blocks, axis=0))
        ds = term if ds is None else ds + term
    limit_row = jnp.zeros((1, wide), jnp.int32)
    req_row = lax.broadcasted_iota(jnp.int32, (1, wide), 1) % reqs
    for r in range(reqs):
        limit_row = jnp.where(req_row == r, dlen[r], limit_row)
    dpos = lax.broadcasted_iota(jnp.int32, (cached, wide), 0)
    ds = jnp.where(dpos < limit_row, ds, NEG)
    dw = jnp.exp2((ds - jnp.max(ds, axis=0, keepdims=True)) * SCALE2)
    dwt = dw.T
    dtotal = jnp.sum(dwt, axis=1, keepdims=True)
    dwt = dwt.astype(jnp.bfloat16)
    row_req = lax.broadcasted_iota(jnp.int32, (wide, HD), 0) % reqs
    part = group * reqs
    dmix = jnp.zeros((wide, HD), jnp.float32)
    for r in range(reqs):
        full = nt(dwt, dkv[1, r])
        picked = jnp.concatenate(
            [full[g * part : (g + 1) * part, g * HD : (g + 1) * HD] for g in range(kvh)], axis=0
        )
        dmix = jnp.where(row_req == r, picked, dmix)
    dmix = dmix / dtotal
    for h in range(heads):
        dout[:, h * HD : (h + 1) * HD] = dmix[h * reqs : (h + 1) * reqs].astype(jnp.bfloat16)

    @pl.when(z < early)
    def _():
        reach_up()

    swap.wait_recv()

    @pl.when(sub == 1)
    def _():
        set_keys([nkv_far.at[0]], [nkv_far.at[1]], [hide((rows, HD), 0, count)])
        attend(False)

    limit = hlen[0]

    def page_of(owner):
        page = 0
        for p in range(ng):
            page = page + jnp.where(place[0, p] == owner, p, 0)
        return page

    def take(b):
        for s in (source_of(2 * b, z, ng), source_of(2 * b + 1, z, ng)):
            arrival(s).wait_recv()
            forward(s).start()

    def use(b, last_block=False):
        order = (2 * b, 2 * b + 1)
        slots = [source_of(j, z, ng) for j in order]
        biases = [
            hide((half, HD), page_of(j) * PAGE + who * half, limit)
            for j in slots
            for who in (sub, 1 - sub)
        ]
        for s in slots:
            forward(s).wait_recv()
        parts = [r.at[s] for s in slots for r in (near, far)]
        set_keys([p.at[0] for p in parts], [p.at[1] for p in parts], biases)
        attend(False, last_block)

    second = source_of(1, z, ng)
    arrival(second).wait_recv()
    forward(second).start()
    pairs = ng // 2

    def pair(b, carry):
        @pl.when(b < pairs - 1)
        def _():
            take(b)

        use(b - 1)

        @pl.when(b == pairs - 1)
        def _():
            take(b)

        return carry

    lax.fori_loop(1, pairs, pair, 0)
    use(pairs - 1, True)

    for d in range(ng):

        @pl.when(z != d)
        def _():
            send(d).wait_send()

        forward(d).wait_send()
    swap.wait_send()


def solution(mesh):
    ng = mesh.shape["grp"]

    def shards(new_q, new_kv, hist_kv, page_place, hist_len, new_len, dec_q, dec_cache, dec_len):
        rows, width = new_q.shape
        heads = width // HD
        kvh = new_kv.shape[2] // HD
        half, lanes = hist_kv.shape[4:]
        keys = 4 * half
        anywhere = pl.BlockSpec(memory_space=pltpu.HBM)
        scalars = pl.BlockSpec(memory_space=pltpu.SMEM)
        vmem = pl.BlockSpec(memory_space=pltpu.VMEM)
        bf16, f32 = jnp.bfloat16, jnp.float32

        def keep(x):
            return pltpu.with_memory_space_constraint(x, pltpu.HBM)

        def kernel(*refs):
            body(ng, *refs)

        return pl.pallas_call(
            kernel,
            name="serve",
            out_shape=(
                jax.ShapeDtypeStruct(new_q.shape, bf16),
                jax.ShapeDtypeStruct(dec_q.shape, bf16),
            ),
            in_specs=[anywhere] * 4 + [scalars] * 2 + [anywhere] * 3,
            out_specs=(vmem, vmem),
            scratch_shapes=[
                pltpu.VMEM(new_q.shape, bf16),
                pltpu.VMEM(new_kv.shape, bf16),
                pltpu.VMEM(new_kv.shape, bf16),
                pltpu.VMEM((2, ng, half, lanes), bf16),
                pltpu.VMEM(dec_q.shape, bf16),
                pltpu.VMEM(dec_cache.shape, bf16),
                pltpu.VMEM((ng, 2, half, lanes), bf16),
                pltpu.VMEM((ng, 2, half, lanes), bf16),
                pltpu.VMEM((heads, 2 * HD, rows), bf16),
                pltpu.VMEM((kvh, keys, 2 * HD), bf16),
                pltpu.VMEM((kvh, HD, keys), bf16),
                pltpu.VMEM((heads, HD, rows), f32),
                pltpu.VMEM((heads, 8, rows), f32),
                pltpu.VMEM((heads, 8, rows), f32),
                pltpu.SMEM(page_place.shape, jnp.int32),
                pltpu.SMEM(dec_len.shape, jnp.int32),
                pltpu.SemaphoreType.DMA((8,)),
                pltpu.SemaphoreType.DMA((ng,)),
                pltpu.SemaphoreType.DMA((ng,)),
                pltpu.SemaphoreType.DMA((ng + 1,)),
                pltpu.SemaphoreType.DMA((ng + 1,)),
                pltpu.SemaphoreType.REGULAR((ng,)),
            ],
            compiler_params=pltpu.CompilerParams(
                collective_id=0, has_side_effects=True, vmem_limit_bytes=40 * 1024 * 1024
            ),
        )(
            *(keep(x) for x in (new_q, new_kv, hist_kv, page_place)),
            hist_len,
            new_len,
            *(keep(x) for x in (dec_q, dec_cache, dec_len)),
        )

    in_specs = (
        P(("rep", "grp", "sub"), "tp"),
        P(None, ("rep", "grp", "sub"), "tp"),
        P(None, ("rep", "grp"), None, None, "sub", "tp"),
        P(("rep", "grp"), None),
        P(("rep", "grp")),
        P(("rep", "grp")),
        P(("rep", "grp", "sub"), "tp"),
        P(None, ("rep", "grp", "sub"), None, "tp"),
        P(("rep", "grp", "sub")),
    )
    out_specs = (P(("rep", "grp", "sub"), "tp"), P(("rep", "grp", "sub"), "tp"))
    return jax.shard_map(shards, mesh=mesh, in_specs=in_specs, out_specs=out_specs, check_vma=False)
```

```python
import math

import jax
import jax.numpy as jnp
from jax import lax
from jax.experimental import pallas as pl
from jax.experimental.pallas import tpu as pltpu
from jax.sharding import PartitionSpec as P

HD = 128
PAGE = 128
NEG = -1e30
MESH = pl.DeviceIdType.MESH
SCALE2 = (HD**-0.5) * math.log2(math.e)


def source_of(j, z, ng):
    odd = j % 2
    step = odd * ((j + 1) // 2) - (1 - odd) * (j // 2)
    return (z + step + ng) % ng


def nt(a, b):
    return lax.dot_general(a, b, (((1,), (0,)), ((), ())), preferred_element_type=jnp.float32)


def body(
    ng,
    q_hbm,
    nkv_hbm,
    hist_hbm,
    place_hbm,
    hlen,
    nlen,
    dq_hbm,
    dkv_hbm,
    dlen_hbm,
    out,
    dout,
    q_v,
    nkv,
    nkv_far,
    hist,
    dq_v,
    dkv,
    near,
    far,
    qt,
    kb,
    vt,
    acc,
    top,
    total,
    place,
    dlen,
    local_sem,
    send_sem,
    recv_sem,
    fsend_sem,
    frecv_sem,
    in_sem,
):
    z = lax.axis_index("grp")
    sub = lax.axis_index("sub")
    heads = qt.shape[0]
    kvh = kb.shape[0]
    group = heads // kvh
    rows = q_v.shape[0]
    half = near.shape[2]
    reqs, cached = dkv.shape[1], dkv.shape[2]

    low = ng // 2
    early = low - 3
    nigh = low + 3
    first = jnp.where(lax.axis_index("tp") == 0, ng - 2, low)
    barrier = pltpu.get_barrier_semaphore()

    def greet(d):
        pl.semaphore_signal(barrier, inc=1, device_id={"grp": d}, device_id_type=MESH)

    def tell(sem, d):
        pl.semaphore_signal(sem, inc=1, device_id={"grp": d}, device_id_type=MESH)

    pl.semaphore_signal(barrier, inc=1, device_id={"sub": 1 - sub}, device_id_type=MESH)

    for d in range(low, ng):

        @pl.when((z == 0) & ((first == low) | (first == d)))
        def _():
            greet(d)

    load_hist = pltpu.make_async_copy(hist_hbm.at[:, 0, :, 0], hist, local_sem.at[0])
    load_own = pltpu.make_async_copy(hist_hbm.at[:, 0, z, 0], near.at[z], local_sem.at[1])
    load_nkv = pltpu.make_async_copy(nkv_hbm, nkv, local_sem.at[2])
    load_q = pltpu.make_async_copy(q_hbm, q_v, local_sem.at[3])
    load_dq = pltpu.make_async_copy(dq_hbm, dq_v, local_sem.at[4])
    load_dkv = pltpu.make_async_copy(dkv_hbm, dkv, local_sem.at[5])
    load_scalars = [
        pltpu.make_async_copy(place_hbm, place, local_sem.at[6]),
        pltpu.make_async_copy(dlen_hbm, dlen, local_sem.at[7]),
    ]
    for load in (load_hist, load_own, load_nkv, load_q, load_dq, *load_scalars, load_dkv):
        load.start()
    load_hist.wait()
    load_own.wait()
    load_nkv.wait()
    pred = jnp.where(z >= 2, 1, 0)
    zero = jnp.where(((first == low) & (z >= low)) | (first == z), 1, 0)
    pl.semaphore_wait(barrier, 1 + pred + zero)

    def send(d):
        return pltpu.make_async_remote_copy(
            src_ref=hist.at[:, d],
            dst_ref=near.at[z],
            send_sem=send_sem.at[d],
            recv_sem=recv_sem.at[z],
            device_id={"grp": d},
            device_id_type=MESH,
        )

    @pl.when((z >= 1) & (z < ng - 1))
    def _():
        greet(z + 1)

    for d in range(ng - 1):

        @pl.when(z >= first if d == 0 else z > d)
        def _():
            tell(in_sem.at[z], d)

    def give(when, d):
        @pl.when(when)
        def _():
            send(d).start()

    for t in range(low):
        straight = (z >= first) | ((first == low) & (z >= low))
        if t > 0:
            straight |= z >= nigh
        give(straight & (t <= z - low), t)
        if t < low - 1:
            down = z - 1 - t
            give((z >= low) | ((z >= 1) & (down >= 1)), down)

    def hear(d):
        pl.semaphore_wait(in_sem.at[d], 1)

    def reach_up():
        for d in range(2, low):

            @pl.when((z >= 1) & (z < d))
            def _():
                hear(d)
                send(d).start()

        hear(first)
        give(z >= 1, 0)
        for t in range(1, low):
            give((z == 0) & (t < first), t)
            if low < ng - 1 - t:
                give((z == 0) & (ng - 1 - t < first), ng - 1 - t)
        give((z == 0) & (low < first), low)
        for d in range(low, ng):

            @pl.when(((z >= 1) | (d >= first)) & (d != first))
            def _():
                hear(d)

            give((z >= 1) | (d >= first), d)

    def forward(s):
        return pltpu.make_async_remote_copy(
            src_ref=near.at[s],
            dst_ref=far.at[s],
            send_sem=fsend_sem.at[s],
            recv_sem=frecv_sem.at[s],
            device_id={"sub": 1 - sub},
            device_id_type=MESH,
        )

    def arrival(s):
        return pltpu.make_async_remote_copy(
            src_ref=near.at[s],
            dst_ref=near.at[s],
            send_sem=send_sem.at[s],
            recv_sem=recv_sem.at[s],
            device_id={"sub": 1 - sub},
            device_id_type=MESH,
        )

    swap = pltpu.make_async_remote_copy(
        src_ref=nkv,
        dst_ref=nkv_far,
        send_sem=fsend_sem.at[ng],
        recv_sem=frecv_sem.at[ng],
        device_id={"sub": 1 - sub},
        device_id_type=MESH,
    )
    swap.start()
    forward(z).start()

    @pl.when(z >= low)
    def _():
        @pl.when((first != low) & (z < first))
        def _():
            hear(first)

        for t in range(low):
            held = (first != low) & (z < first) & (t <= z - low)
            give(held if t == 0 else held & (z < nigh), t)
        for d in range(low + 1, ng):

            @pl.when((z < d) & (d != first))
            def _():
                hear(d)

            give(z < d, d)

    @pl.when((z >= early) & (z < low))
    def _():
        reach_up()


    load_q.wait()
    for load in load_scalars:
        load.wait()
    one_row = (lax.broadcasted_iota(jnp.int32, (HD, rows), 0) == 0).astype(jnp.float32)
    one_row = one_row.astype(jnp.bfloat16)
    for h in range(heads):
        scaled = q_v[:, h * HD : (h + 1) * HD].astype(jnp.float32) * SCALE2
        qt[h, :HD] = scaled.T.astype(jnp.bfloat16)
        qt[h, HD:] = one_row
    top[...] = jnp.full_like(top, NEG)
    total[...] = jnp.zeros_like(total)
    acc[...] = jnp.zeros_like(acc)

    def set_keys(keys, values, biases):
        for g in range(kvh):
            lanes = slice(g * HD, (g + 1) * HD)
            kb[g, :, :HD] = jnp.concatenate([r[:, lanes] for r in keys], axis=0)
            kb[g, :, HD:] = jnp.concatenate(biases, axis=0)
            v = jnp.concatenate([r[:, lanes] for r in values], axis=0)
            vt[g] = v.astype(jnp.float32).T.astype(jnp.bfloat16)

    span = kb.shape[1]

    def attend(causal, last_block=False):
        def score(h):
            s = nt(kb[h // group], qt[h])
            if causal:
                key = lax.broadcasted_iota(jnp.int32, s.shape, 0)
                query = lax.broadcasted_iota(jnp.int32, s.shape, 1)
                s = jnp.where(key <= query, s, NEG)
            return s.reshape(span // 8, 8, rows)

        def weigh(h, s):
            old = top[h]
            new = jnp.maximum(old, jnp.max(s, axis=0))
            for shift in (4, 2, 1):
                new = jnp.maximum(new, pltpu.roll(new, shift, 0))
            fade = jnp.exp2(old - new)
            w = jnp.exp2(s - new[None])
            top[h] = new
            total[h] = total[h] * fade + jnp.sum(w, axis=0)
            return w.reshape(span, rows).astype(jnp.bfloat16), fade

        def mix(h, w, fade):
            kept = acc[h].reshape(HD // 8, 8, rows) * fade[None]
            mixed = kept.reshape(HD, rows) + nt(vt[h // group], w)
            if last_block:
                mixed = mixed / jnp.sum(total[h], axis=0, keepdims=True)
                mixed = jnp.where(live, mixed, 0.0)
                out[:, h * HD : (h + 1) * HD] = mixed.T.astype(jnp.bfloat16)
            else:
                acc[h] = mixed

        s = score(0)
        last = None
        for h in range(heads):
            ahead = score(h + 1) if h + 1 < heads else None
            w, fade = weigh(h, s)
            if last is not None:
                mix(*last)
            last = (h, w, fade)
            s = ahead
        mix(*last)

    count = nlen[0]
    live = sub * rows + lax.broadcasted_iota(jnp.int32, (1, rows), 1) < count

    def hide(shape, start, limit):
        position = start + lax.broadcasted_iota(jnp.int32, shape, 0)
        return jnp.where(position < limit, 0.0, NEG).astype(jnp.bfloat16)

    set_keys([nkv.at[0]], [nkv.at[1]], [hide((rows, HD), sub * rows, count)])
    attend(True)

    load_dq.wait()
    load_dkv.wait()
    dq = dq_v[...].astype(jnp.float32)
    wide = heads * reqs
    dq_rows = jnp.concatenate([dq[:, h * HD : (h + 1) * HD] for h in range(heads)], axis=0)
    dq_cols = dq_rows.T
    col = lax.broadcasted_iota(jnp.int32, (HD, wide), 1)
    col_req = col % reqs
    col_kv = col // (reqs * group)
    ds = None
    for r in range(reqs):
        blocks = [
            jnp.where((col_req == r) & (col_kv == g), dq_cols, 0.0).astype(jnp.bfloat16)
            for g in range(kvh)
        ]
        term = nt(dkv[0, r], jnp.concatenate(blocks, axis=0))
        ds = term if ds is None else ds + term
    limit_row = jnp.zeros((1, wide), jnp.int32)
    req_row = lax.broadcasted_iota(jnp.int32, (1, wide), 1) % reqs
    for r in range(reqs):
        limit_row = jnp.where(req_row == r, dlen[r], limit_row)
    dpos = lax.broadcasted_iota(jnp.int32, (cached, wide), 0)
    ds = jnp.where(dpos < limit_row, ds, NEG)
    dw = jnp.exp2((ds - jnp.max(ds, axis=0, keepdims=True)) * SCALE2)
    dwt = dw.T
    dtotal = jnp.sum(dwt, axis=1, keepdims=True)
    dwt = dwt.astype(jnp.bfloat16)
    row_req = lax.broadcasted_iota(jnp.int32, (wide, HD), 0) % reqs
    part = group * reqs
    dmix = jnp.zeros((wide, HD), jnp.float32)
    for r in range(reqs):
        full = nt(dwt, dkv[1, r])
        picked = jnp.concatenate(
            [full[g * part : (g + 1) * part, g * HD : (g + 1) * HD] for g in range(kvh)], axis=0
        )
        dmix = jnp.where(row_req == r, picked, dmix)
    dmix = dmix / dtotal
    for h in range(heads):
        dout[:, h * HD : (h + 1) * HD] = dmix[h * reqs : (h + 1) * reqs].astype(jnp.bfloat16)

    @pl.when(z < early)
    def _():
        reach_up()

    swap.wait_recv()

    @pl.when(sub == 1)
    def _():
        set_keys([nkv_far.at[0]], [nkv_far.at[1]], [hide((rows, HD), 0, count)])
        attend(False)

    limit = hlen[0]

    def page_of(owner):
        page = 0
        for p in range(ng):
            page = page + jnp.where(place[0, p] == owner, p, 0)
        return page

    def take(b):
        for s in (source_of(2 * b, z, ng), source_of(2 * b + 1, z, ng)):
            arrival(s).wait_recv()
            forward(s).start()

    def use(b, last_block=False):
        order = (2 * b, 2 * b + 1)
        slots = [source_of(j, z, ng) for j in order]
        biases = [
            hide((half, HD), page_of(j) * PAGE + who * half, limit)
            for j in slots
            for who in (sub, 1 - sub)
        ]
        for s in slots:
            forward(s).wait_recv()
        parts = [r.at[s] for s in slots for r in (near, far)]
        set_keys([p.at[0] for p in parts], [p.at[1] for p in parts], biases)
        attend(False, last_block)

    second = source_of(1, z, ng)
    arrival(second).wait_recv()
    forward(second).start()
    pairs = ng // 2

    def pair(b, carry):
        @pl.when(b < pairs - 1)
        def _():
            take(b)

        use(b - 1)

        @pl.when(b == pairs - 1)
        def _():
            take(b)

        return carry

    lax.fori_loop(1, pairs, pair, 0)
    use(pairs - 1, True)

    for d in range(ng):

        @pl.when(z != d)
        def _():
            send(d).wait_send()

        forward(d).wait_send()
    swap.wait_send()


def solution(mesh):
    ng = mesh.shape["grp"]

    def shards(new_q, new_kv, hist_kv, page_place, hist_len, new_len, dec_q, dec_cache, dec_len):
        rows, width = new_q.shape
        heads = width // HD
        kvh = new_kv.shape[2] // HD
        half, lanes = hist_kv.shape[4:]
        keys = 4 * half
        anywhere = pl.BlockSpec(memory_space=pltpu.HBM)
        scalars = pl.BlockSpec(memory_space=pltpu.SMEM)
        vmem = pl.BlockSpec(memory_space=pltpu.VMEM)
        bf16, f32 = jnp.bfloat16, jnp.float32

        def keep(x):
            return pltpu.with_memory_space_constraint(x, pltpu.HBM)

        def kernel(*refs):
            body(ng, *refs)

        return pl.pallas_call(
            kernel,
            name="serve",
            out_shape=(
                jax.ShapeDtypeStruct(new_q.shape, bf16),
                jax.ShapeDtypeStruct(dec_q.shape, bf16),
            ),
            in_specs=[anywhere] * 4 + [scalars] * 2 + [anywhere] * 3,
            out_specs=(vmem, vmem),
            scratch_shapes=[
                pltpu.VMEM(new_q.shape, bf16),
                pltpu.VMEM(new_kv.shape, bf16),
                pltpu.VMEM(new_kv.shape, bf16),
                pltpu.VMEM((2, ng, half, lanes), bf16),
                pltpu.VMEM(dec_q.shape, bf16),
                pltpu.VMEM(dec_cache.shape, bf16),
                pltpu.VMEM((ng, 2, half, lanes), bf16),
                pltpu.VMEM((ng, 2, half, lanes), bf16),
                pltpu.VMEM((heads, 2 * HD, rows), bf16),
                pltpu.VMEM((kvh, keys, 2 * HD), bf16),
                pltpu.VMEM((kvh, HD, keys), bf16),
                pltpu.VMEM((heads, HD, rows), f32),
                pltpu.VMEM((heads, 8, rows), f32),
                pltpu.VMEM((heads, 8, rows), f32),
                pltpu.SMEM(page_place.shape, jnp.int32),
                pltpu.SMEM(dec_len.shape, jnp.int32),
                pltpu.SemaphoreType.DMA((8,)),
                pltpu.SemaphoreType.DMA((ng,)),
                pltpu.SemaphoreType.DMA((ng,)),
                pltpu.SemaphoreType.DMA((ng + 1,)),
                pltpu.SemaphoreType.DMA((ng + 1,)),
                pltpu.SemaphoreType.REGULAR((ng,)),
            ],
            compiler_params=pltpu.CompilerParams(
                collective_id=0, has_side_effects=True, vmem_limit_bytes=40 * 1024 * 1024
            ),
        )(
            *(keep(x) for x in (new_q, new_kv, hist_kv, page_place)),
            hist_len,
            new_len,
            *(keep(x) for x in (dec_q, dec_cache, dec_len)),
        )

    in_specs = (
        P(("rep", "grp", "sub"), "tp"),
        P(None, ("rep", "grp", "sub"), "tp"),
        P(None, ("rep", "grp"), None, None, "sub", "tp"),
        P(("rep", "grp"), None),
        P(("rep", "grp")),
        P(("rep", "grp")),
        P(("rep", "grp", "sub"), "tp"),
        P(None, ("rep", "grp", "sub"), None, "tp"),
        P(("rep", "grp", "sub")),
    )
    out_specs = (P(("rep", "grp", "sub"), "tp"), P(("rep", "grp", "sub"), "tp"))
    return jax.shard_map(shards, mesh=mesh, in_specs=in_specs, out_specs=out_specs, check_vma=False)
```

```python
import math

import jax
import jax.numpy as jnp
from jax import lax
from jax.experimental import pallas as pl
from jax.experimental.pallas import tpu as pltpu
from jax.sharding import PartitionSpec as P

HD = 128
PAGE = 128
NEG = -1e30
MESH = pl.DeviceIdType.MESH
SCALE2 = (HD**-0.5) * math.log2(math.e)


def source_of(j, z, ng):
    odd = j % 2
    step = odd * ((j + 1) // 2) - (1 - odd) * (j // 2)
    return (z + step + ng) % ng


def nt(a, b):
    return lax.dot_general(a, b, (((1,), (0,)), ((), ())), preferred_element_type=jnp.float32)


def body(
    ng,
    q_hbm,
    nkv_hbm,
    hist_hbm,
    place_hbm,
    hlen,
    nlen,
    dq_hbm,
    dkv_hbm,
    dlen_hbm,
    out,
    dout,
    q_v,
    nkv,
    nkv_far,
    hist,
    dq_v,
    dkv,
    near,
    far,
    qt,
    kb,
    vt,
    acc,
    top,
    total,
    place,
    dlen,
    local_sem,
    send_sem,
    recv_sem,
    fsend_sem,
    frecv_sem,
    in_sem,
):
    z = lax.axis_index("grp")
    sub = lax.axis_index("sub")
    heads = qt.shape[0]
    kvh = kb.shape[0]
    group = heads // kvh
    rows = q_v.shape[0]
    half = near.shape[2]
    reqs, cached = dkv.shape[1], dkv.shape[2]

    low = ng // 2
    early = low - 3
    first = jnp.where(lax.axis_index("tp") == 0, ng - 2, low)
    barrier = pltpu.get_barrier_semaphore()

    def greet(d):
        pl.semaphore_signal(barrier, inc=1, device_id={"grp": d}, device_id_type=MESH)

    def tell(sem, d):
        pl.semaphore_signal(sem, inc=1, device_id={"grp": d}, device_id_type=MESH)

    pl.semaphore_signal(barrier, inc=1, device_id={"sub": 1 - sub}, device_id_type=MESH)

    for d in range(low, ng):

        @pl.when((z == 0) & ((first == low) | (first == d)))
        def _():
            greet(d)

    load_hist = pltpu.make_async_copy(hist_hbm.at[:, 0, :, 0], hist, local_sem.at[0])
    load_own = pltpu.make_async_copy(hist_hbm.at[:, 0, z, 0], near.at[z], local_sem.at[1])
    load_nkv = pltpu.make_async_copy(nkv_hbm, nkv, local_sem.at[2])
    load_q = pltpu.make_async_copy(q_hbm, q_v, local_sem.at[3])
    load_dq = pltpu.make_async_copy(dq_hbm, dq_v, local_sem.at[4])
    load_dkv = pltpu.make_async_copy(dkv_hbm, dkv, local_sem.at[5])
    load_scalars = [
        pltpu.make_async_copy(place_hbm, place, local_sem.at[6]),
        pltpu.make_async_copy(dlen_hbm, dlen, local_sem.at[7]),
    ]
    for load in (load_hist, load_own, load_nkv, load_q, load_dq, *load_scalars, load_dkv):
        load.start()
    load_hist.wait()
    load_own.wait()
    load_nkv.wait()
    pred = jnp.where(z >= 2, 1, 0)
    zero = jnp.where(((first == low) & (z >= low)) | (first == z), 1, 0)
    pl.semaphore_wait(barrier, 1 + pred + zero)

    def send(d):
        return pltpu.make_async_remote_copy(
            src_ref=hist.at[:, d],
            dst_ref=near.at[z],
            send_sem=send_sem.at[d],
            recv_sem=recv_sem.at[z],
            device_id={"grp": d},
            device_id_type=MESH,
        )

    @pl.when((z >= 1) & (z < ng - 1))
    def _():
        greet(z + 1)

    for d in range(ng - 1):

        @pl.when(z >= first if d == 0 else z > d)
        def _():
            tell(in_sem.at[z], d)

    def give(when, d):
        @pl.when(when)
        def _():
            send(d).start()

    for t in range(low):
        straight = (z >= first) | ((first == low) & (z >= low))
        give(straight & (t <= z - low), t)
        if t < low - 1:
            down = z - 1 - t
            give((z >= low) | ((z >= 1) & (down >= 1)), down)

    def hear(d):
        pl.semaphore_wait(in_sem.at[d], 1)

    def reach_up():
        for d in range(2, low):

            @pl.when((z >= 1) & (z < d))
            def _():
                hear(d)
                send(d).start()

        soon = (first == low) | (z == 0) | (z >= early)
        later = jnp.logical_not(soon)

        @pl.when(soon)
        def _():
            hear(first)

        give(soon & (z >= 1), 0)
        for t in range(1, low):
            give((z == 0) & (t < first), t)
            if low < ng - 1 - t:
                give((z == 0) & (ng - 1 - t < first), ng - 1 - t)
        give((z == 0) & (low < first), low)
        for d in range(low, ng):

            @pl.when(((z >= 1) | (d >= first)) & ((d != first) | later))
            def _():
                hear(d)

            give((z >= 1) | (d >= first), d)
            if d == ng - 2:
                give(later, 0)

    def forward(s):
        return pltpu.make_async_remote_copy(
            src_ref=near.at[s],
            dst_ref=far.at[s],
            send_sem=fsend_sem.at[s],
            recv_sem=frecv_sem.at[s],
            device_id={"sub": 1 - sub},
            device_id_type=MESH,
        )

    def arrival(s):
        return pltpu.make_async_remote_copy(
            src_ref=near.at[s],
            dst_ref=near.at[s],
            send_sem=send_sem.at[s],
            recv_sem=recv_sem.at[s],
            device_id={"sub": 1 - sub},
            device_id_type=MESH,
        )

    swap = pltpu.make_async_remote_copy(
        src_ref=nkv,
        dst_ref=nkv_far,
        send_sem=fsend_sem.at[ng],
        recv_sem=frecv_sem.at[ng],
        device_id={"sub": 1 - sub},
        device_id_type=MESH,
    )
    swap.start()
    forward(z).start()

    @pl.when(z >= low)
    def _():
        @pl.when((first != low) & (z < first))
        def _():
            hear(first)

        for t in range(low):
            give((first != low) & (z < first) & (t <= z - low), t)
        for d in range(low + 1, ng):

            @pl.when((z < d) & (d != first))
            def _():
                hear(d)

            give(z < d, d)

    @pl.when((z >= early) & (z < low))
    def _():
        reach_up()


    load_q.wait()
    for load in load_scalars:
        load.wait()
    one_row = (lax.broadcasted_iota(jnp.int32, (HD, rows), 0) == 0).astype(jnp.float32)
    one_row = one_row.astype(jnp.bfloat16)
    for h in range(heads):
        scaled = q_v[:, h * HD : (h + 1) * HD].astype(jnp.float32) * SCALE2
        qt[h, :HD] = scaled.T.astype(jnp.bfloat16)
        qt[h, HD:] = one_row
    top[...] = jnp.full_like(top, NEG)
    total[...] = jnp.zeros_like(total)
    acc[...] = jnp.zeros_like(acc)

    def set_keys(keys, values, biases):
        for g in range(kvh):
            lanes = slice(g * HD, (g + 1) * HD)
            kb[g, :, :HD] = jnp.concatenate([r[:, lanes] for r in keys], axis=0)
            kb[g, :, HD:] = jnp.concatenate(biases, axis=0)
            v = jnp.concatenate([r[:, lanes] for r in values], axis=0)
            vt[g] = v.astype(jnp.float32).T.astype(jnp.bfloat16)

    span = kb.shape[1]

    def attend(causal, last_block=False):
        def score(h):
            s = nt(kb[h // group], qt[h])
            if causal:
                key = lax.broadcasted_iota(jnp.int32, s.shape, 0)
                query = lax.broadcasted_iota(jnp.int32, s.shape, 1)
                s = jnp.where(key <= query, s, NEG)
            return s.reshape(span // 8, 8, rows)

        def weigh(h, s):
            old = top[h]
            new = jnp.maximum(old, jnp.max(s, axis=0))
            for shift in (4, 2, 1):
                new = jnp.maximum(new, pltpu.roll(new, shift, 0))
            fade = jnp.exp2(old - new)
            w = jnp.exp2(s - new[None])
            top[h] = new
            total[h] = total[h] * fade + jnp.sum(w, axis=0)
            return w.reshape(span, rows).astype(jnp.bfloat16), fade

        def mix(h, w, fade):
            kept = acc[h].reshape(HD // 8, 8, rows) * fade[None]
            mixed = kept.reshape(HD, rows) + nt(vt[h // group], w)
            if last_block:
                mixed = mixed / jnp.sum(total[h], axis=0, keepdims=True)
                mixed = jnp.where(live, mixed, 0.0)
                out[:, h * HD : (h + 1) * HD] = mixed.T.astype(jnp.bfloat16)
            else:
                acc[h] = mixed

        s = score(0)
        last = None
        for h in range(heads):
            ahead = score(h + 1) if h + 1 < heads else None
            w, fade = weigh(h, s)
            if last is not None:
                mix(*last)
            last = (h, w, fade)
            s = ahead
        mix(*last)

    count = nlen[0]
    live = sub * rows + lax.broadcasted_iota(jnp.int32, (1, rows), 1) < count

    def hide(shape, start, limit):
        position = start + lax.broadcasted_iota(jnp.int32, shape, 0)
        return jnp.where(position < limit, 0.0, NEG).astype(jnp.bfloat16)

    set_keys([nkv.at[0]], [nkv.at[1]], [hide((rows, HD), sub * rows, count)])
    attend(True)

    load_dq.wait()
    load_dkv.wait()
    dq = dq_v[...].astype(jnp.float32)
    wide = heads * reqs
    dq_rows = jnp.concatenate([dq[:, h * HD : (h + 1) * HD] for h in range(heads)], axis=0)
    dq_cols = dq_rows.T
    col = lax.broadcasted_iota(jnp.int32, (HD, wide), 1)
    col_req = col % reqs
    col_kv = col // (reqs * group)
    ds = None
    for r in range(reqs):
        blocks = [
            jnp.where((col_req == r) & (col_kv == g), dq_cols, 0.0).astype(jnp.bfloat16)
            for g in range(kvh)
        ]
        term = nt(dkv[0, r], jnp.concatenate(blocks, axis=0))
        ds = term if ds is None else ds + term
    limit_row = jnp.zeros((1, wide), jnp.int32)
    req_row = lax.broadcasted_iota(jnp.int32, (1, wide), 1) % reqs
    for r in range(reqs):
        limit_row = jnp.where(req_row == r, dlen[r], limit_row)
    dpos = lax.broadcasted_iota(jnp.int32, (cached, wide), 0)
    ds = jnp.where(dpos < limit_row, ds, NEG)
    dw = jnp.exp2((ds - jnp.max(ds, axis=0, keepdims=True)) * SCALE2)
    dwt = dw.T
    dtotal = jnp.sum(dwt, axis=1, keepdims=True)
    dwt = dwt.astype(jnp.bfloat16)
    row_req = lax.broadcasted_iota(jnp.int32, (wide, HD), 0) % reqs
    part = group * reqs
    dmix = jnp.zeros((wide, HD), jnp.float32)
    for r in range(reqs):
        full = nt(dwt, dkv[1, r])
        picked = jnp.concatenate(
            [full[g * part : (g + 1) * part, g * HD : (g + 1) * HD] for g in range(kvh)], axis=0
        )
        dmix = jnp.where(row_req == r, picked, dmix)
    dmix = dmix / dtotal
    for h in range(heads):
        dout[:, h * HD : (h + 1) * HD] = dmix[h * reqs : (h + 1) * reqs].astype(jnp.bfloat16)

    @pl.when(z < early)
    def _():
        reach_up()

    swap.wait_recv()

    @pl.when(sub == 1)
    def _():
        set_keys([nkv_far.at[0]], [nkv_far.at[1]], [hide((rows, HD), 0, count)])
        attend(False)

    limit = hlen[0]

    def page_of(owner):
        page = 0
        for p in range(ng):
            page = page + jnp.where(place[0, p] == owner, p, 0)
        return page

    def take(b):
        for s in (source_of(2 * b, z, ng), source_of(2 * b + 1, z, ng)):
            arrival(s).wait_recv()
            forward(s).start()

    def use(b, last_block=False):
        order = (2 * b, 2 * b + 1)
        slots = [source_of(j, z, ng) for j in order]
        biases = [
            hide((half, HD), page_of(j) * PAGE + who * half, limit)
            for j in slots
            for who in (sub, 1 - sub)
        ]
        for s in slots:
            forward(s).wait_recv()
        parts = [r.at[s] for s in slots for r in (near, far)]
        set_keys([p.at[0] for p in parts], [p.at[1] for p in parts], biases)
        attend(False, last_block)

    second = source_of(1, z, ng)
    arrival(second).wait_recv()
    forward(second).start()
    pairs = ng // 2

    def pair(b, carry):
        @pl.when(b < pairs - 1)
        def _():
            take(b)

        use(b - 1)

        @pl.when(b == pairs - 1)
        def _():
            take(b)

        return carry

    lax.fori_loop(1, pairs, pair, 0)
    use(pairs - 1, True)

    for d in range(ng):

        @pl.when(z != d)
        def _():
            send(d).wait_send()

        forward(d).wait_send()
    swap.wait_send()


def solution(mesh):
    ng = mesh.shape["grp"]

    def shards(new_q, new_kv, hist_kv, page_place, hist_len, new_len, dec_q, dec_cache, dec_len):
        rows, width = new_q.shape
        heads = width // HD
        kvh = new_kv.shape[2] // HD
        half, lanes = hist_kv.shape[4:]
        keys = 4 * half
        anywhere = pl.BlockSpec(memory_space=pltpu.HBM)
        scalars = pl.BlockSpec(memory_space=pltpu.SMEM)
        vmem = pl.BlockSpec(memory_space=pltpu.VMEM)
        bf16, f32 = jnp.bfloat16, jnp.float32

        def keep(x):
            return pltpu.with_memory_space_constraint(x, pltpu.HBM)

        def kernel(*refs):
            body(ng, *refs)

        return pl.pallas_call(
            kernel,
            name="serve",
            out_shape=(
                jax.ShapeDtypeStruct(new_q.shape, bf16),
                jax.ShapeDtypeStruct(dec_q.shape, bf16),
            ),
            in_specs=[anywhere] * 4 + [scalars] * 2 + [anywhere] * 3,
            out_specs=(vmem, vmem),
            scratch_shapes=[
                pltpu.VMEM(new_q.shape, bf16),
                pltpu.VMEM(new_kv.shape, bf16),
                pltpu.VMEM(new_kv.shape, bf16),
                pltpu.VMEM((2, ng, half, lanes), bf16),
                pltpu.VMEM(dec_q.shape, bf16),
                pltpu.VMEM(dec_cache.shape, bf16),
                pltpu.VMEM((ng, 2, half, lanes), bf16),
                pltpu.VMEM((ng, 2, half, lanes), bf16),
                pltpu.VMEM((heads, 2 * HD, rows), bf16),
                pltpu.VMEM((kvh, keys, 2 * HD), bf16),
                pltpu.VMEM((kvh, HD, keys), bf16),
                pltpu.VMEM((heads, HD, rows), f32),
                pltpu.VMEM((heads, 8, rows), f32),
                pltpu.VMEM((heads, 8, rows), f32),
                pltpu.SMEM(page_place.shape, jnp.int32),
                pltpu.SMEM(dec_len.shape, jnp.int32),
                pltpu.SemaphoreType.DMA((8,)),
                pltpu.SemaphoreType.DMA((ng,)),
                pltpu.SemaphoreType.DMA((ng,)),
                pltpu.SemaphoreType.DMA((ng + 1,)),
                pltpu.SemaphoreType.DMA((ng + 1,)),
                pltpu.SemaphoreType.REGULAR((ng,)),
            ],
            compiler_params=pltpu.CompilerParams(
                collective_id=0, has_side_effects=True, vmem_limit_bytes=40 * 1024 * 1024
            ),
        )(
            *(keep(x) for x in (new_q, new_kv, hist_kv, page_place)),
            hist_len,
            new_len,
            *(keep(x) for x in (dec_q, dec_cache, dec_len)),
        )

    in_specs = (
        P(("rep", "grp", "sub"), "tp"),
        P(None, ("rep", "grp", "sub"), "tp"),
        P(None, ("rep", "grp"), None, None, "sub", "tp"),
        P(("rep", "grp"), None),
        P(("rep", "grp")),
        P(("rep", "grp")),
        P(("rep", "grp", "sub"), "tp"),
        P(None, ("rep", "grp", "sub"), None, "tp"),
        P(("rep", "grp", "sub")),
    )
    out_specs = (P(("rep", "grp", "sub"), "tp"), P(("rep", "grp", "sub"), "tp"))
    return jax.shard_map(shards, mesh=mesh, in_specs=in_specs, out_specs=out_specs, check_vma=False)
```
